32 devices in a mesh: chain: 4 (over y, core), cols: 8 (over z, x).
Axes of the slice: x: 2, y: 2, z: 4, core: 2. Of those that a mesh axis runs over, the one named last changes fastest.
Arguments:
- factor: float32 [4608, 4608], P(('chain', 'cols')), may hold values from -2 to 2, as said below
- right_side: float32 [4608, 1024], P('chain', 'cols'), may hold values from -6 to 6
- occ_order: int32 [16], replicated, may hold values from 0 to 15, each once
- cabs_order: int32 [64], replicated, may hold values from 0 to 63, each once
Outputs:
- fitted: float32 [16, 64, 4608], P('cols', None, 'chain')
The draws below stay inside these ranges and needn't reach their ends.
Inputs may be any that keep to these rules, and one draw needn't show every extreme that they name: factor is lower triangular: zero above the diagonal, its diagonal between 1 and 2.
All inputs are finite; a program needn't handle non-finite values.
Results may differ from the reference program's by a relative error of at most 0.00017.
Values sent between devices are 32-bit elements; how exact they have to be, the bound alone decides.
A program may use at most 128 MiB of HBM per device.

```python
import math
import jax
import jax.numpy as jnp

NAUX = 4608
CABSW = 64
OCCW = 16
NCOL = 1024


def draw_factor(key, part):
    key_off = jax.random.fold_in(key, 11)
    key_diag = jax.random.fold_in(key, 12)
    off_diag = jnp.clip(jax.random.normal(key_off, (NAUX, NAUX), jnp.float32), -6.0, 6.0)
    off_diag = jnp.tril(off_diag * (2.5 / math.sqrt(NAUX)), -1)
    diag_vals = jax.random.uniform(key_diag, (NAUX,), jnp.float32, 1.0, 2.0)
    return off_diag + jnp.diag(diag_vals)


def block_scale(stream_key, shape, split, low, high):
    level, own = 1.0, jax.random.fold_in(stream_key, 6)
    for position, parts in split:
        steps = jnp.exp(jax.random.uniform(jax.random.fold_in(own, position), (parts,), jnp.float32, low / len(split), high / len(split)))
        level = level * jnp.repeat(steps, shape[position] // parts).reshape([-1 if axis == position else 1 for axis in range(len(shape))])
    return level


def gaussian(own_key, shape, width, bound, cuts=(), kind=jnp.bfloat16):
    drawn = width * jax.random.normal(own_key, shape, jnp.float32)
    if cuts:
        drawn = drawn * block_scale(own_key, shape, cuts, -0.22, 0.18)
    return jnp.clip(drawn, -bound, bound).astype(kind)


def setup_inputs(seed: int = 0) -> dict:
    keys = jax.random.split(jax.random.key(seed), 5)
    factor = draw_factor(jax.random.fold_in(keys[4], 71), 0)
    right_side = gaussian(keys[1], (NAUX, NCOL), 1.0, 6.0, ((0, 4), (1, 8)), jnp.float32)
    occ_order = jax.random.permutation(keys[2], OCCW).astype(jnp.int32)
    cabs_order = jax.random.permutation(keys[3], CABSW).astype(jnp.int32)
    return {"factor": factor, "right_side": right_side, "occ_order": occ_order, "cabs_order": cabs_order}


def reference(factor, right_side, occ_order, cabs_order):
    solution = jax.scipy.linalg.solve_triangular(factor, right_side, lower=True)
    grid = solution.reshape(NAUX, CABSW, OCCW)
    grid = jnp.take(grid, cabs_order.astype(jnp.int32), axis=1)
    grid = jnp.take(grid, occ_order.astype(jnp.int32), axis=2)
    return jnp.transpose(grid, (2, 1, 0))
```

```python
import functools

import jax
import jax.numpy as jnp
from jax import lax
from jax.experimental import pallas as pl
from jax.experimental.pallas import tpu as pltpu
from jax.sharding import PartitionSpec as P

BLOCK = 128
PIECE = 8
MESH = pl.DeviceIdType.MESH


def from_root(value, axis, source):
    kept = jnp.where(lax.axis_index(axis) == source, value, 0).astype(value.dtype)
    return lax.psum(kept, axis)


def product(left, right):
    return jnp.dot(left, right, precision=lax.Precision.HIGHEST, preferred_element_type=jnp.float32)


def general(factor, right_side, occ_order, cabs_order):
    chain_size = lax.axis_size("chain")
    position = lax.axis_index("chain")
    factor_row = lax.all_gather(factor, "cols", axis=0, tiled=True)
    aux_rows = factor_row.shape[0]
    diag_block = lax.dynamic_slice_in_dim(factor_row, position * aux_rows, aux_rows, 1)
    identity = jnp.eye(aux_rows, dtype=jnp.float32)
    inverse = jax.scipy.linalg.solve_triangular(diag_block, identity, lower=True)

    def settle(residual):
        return product(inverse, residual)

    def blank(residual):
        return jnp.zeros_like(residual)

    residual = right_side
    solution = jnp.zeros_like(right_side)
    for section in range(chain_size):
        solved = lax.cond(position == section, settle, blank, residual)
        solution = solution + solved
        if section + 1 < chain_size:
            arrived = from_root(solved, "chain", section)
            coupling = factor_row[:, section * aux_rows : (section + 1) * aux_rows]

            def lower_block(current, arrived=arrived, coupling=coupling):
                return current - product(coupling, arrived)

            def keep_block(current):
                return current

            residual = lax.cond(position > section, lower_block, keep_block, residual)
    occ_total = occ_order.shape[0]
    cabs_local = right_side.shape[1] // occ_total
    cols_size = lax.axis_size("cols")
    occ_local = occ_total // cols_size
    grid = solution.reshape(aux_rows, cabs_local, occ_total)
    grid = jnp.take(grid, occ_order, axis=2)
    grid = grid.reshape(aux_rows, cabs_local, cols_size, occ_local)
    grid = jnp.transpose(grid, (2, 3, 1, 0))
    moved = jnp.take(
        lax.all_to_all(grid, "cols", split_axis=0, concat_axis=2, tiled=True), cabs_order, axis=2
    )
    return moved.reshape(occ_local, moved.shape[2], aux_rows)


def times_t(left, right, exact=False):
    precision = lax.Precision.HIGHEST
    dims = (((1,), (1,)), ((), ()))
    if exact:
        return lax.dot_general(left, right, dims, precision=precision, preferred_element_type=jnp.float32)
    left_hi = left.astype(jnp.bfloat16)
    left_lo = (left - left_hi.astype(jnp.float32)).astype(jnp.bfloat16)
    right_hi = right.astype(jnp.bfloat16)
    right_lo = (right - right_hi.astype(jnp.float32)).astype(jnp.bfloat16)
    dot = functools.partial(lax.dot_general, dimension_numbers=dims, preferred_element_type=jnp.float32)
    return dot(left_hi, right_hi) + (dot(left_hi, right_lo) + dot(left_lo, right_hi))


def plain(left, right):
    return jnp.dot(left, right, precision=lax.Precision.HIGHEST, preferred_element_type=jnp.float32)


def kernel(
    chains, ring, strip_ref, rhs_ref, out_ref, rows, resid, solved, inverse,
    send, recv, chain_send, chain_recv, rhs_send, rhs_recv, local_sem,
):
    cols = 2 * ring
    strip = strip_ref.shape[0]
    aux = strip * cols
    blocks = aux // BLOCK
    cabs_local = rhs_ref.shape[2]
    width = out_ref.shape[0] * out_ref.shape[1]
    me = lax.axis_index("chain")
    k = lax.axis_index("cols")
    z = k // 2
    x = k % 2
    up, down, far = (z + 1) % ring, (z + ring - 1) % ring, (z + 2) % ring
    partner = 2 * z + (1 - x)
    above, below = 2 * up + x, 2 * down + x

    units = strip // PIECE
    near_half = (units * 5 // 9 // 2) * PIECE
    near = 2 * near_half
    far_half = (strip - near) // 2
    tail = near + far_half

    def slot(zz, xx, begin, size, q):
        start = pl.multiple_of((2 * zz + xx) * strip + begin, PIECE)
        column = me if q == 0 else q - 1
        return rows.at[pl.ds(start, size), pl.ds(pl.multiple_of(column * aux, BLOCK), aux)]

    def push(q, i, zz, xx, begin, size, to):
        ref = slot(zz, xx, begin, size, q)
        return pltpu.make_async_remote_copy(
            src_ref=ref, dst_ref=ref, send_sem=send.at[q, i], recv_sem=recv.at[q, i],
            device_id=(me, to), device_id_type=MESH,
        )

    def sends(q):
        other = 1 - x
        return {
            0: (z, x, 0, strip, partner),
            1: (z, x, 0, strip, above),
            2: (z, x, 0, strip, below),
            3: (z, other, 0, near, above),
            4: (z, other, 0, near, below),
            5: (down, x, near_half, near_half + far_half, above),
            6: (up, x, 0, near_half, below),
            7: (down, other, near_half, near_half, above),
            8: (up, other, 0, near_half, below),
            9: (up, x, tail, far_half, below),
            10: (down, x, near, 2 * far_half, partner),
            11: (up, x, near, 2 * far_half, partner),
            12: (far, x, near, far_half, partner),
            13: (far, x, tail, far_half, partner),
        }

    def arrivals(q):
        other = 1 - x
        return {
            0: (z, other, 0, strip, partner),
            1: (down, x, 0, strip, below),
            2: (up, x, 0, strip, above),
            3: (down, other, 0, near, below),
            4: (up, other, 0, near, above),
            5: (far, x, near_half, near_half + far_half, below),
            6: (far, x, 0, near_half, above),
            7: (far, other, near_half, near_half, below),
            8: (far, other, 0, near_half, above),
            9: (far, x, tail, far_half, above),
            10: (down, other, near, 2 * far_half, partner),
            11: (up, other, near, 2 * far_half, partner),
            12: (far, other, near, far_half, partner),
            13: (far, other, tail, far_half, partner),
        }

    def start(q, i):
        push(q, i, *sends(q)[i]).start()

    def take(q, i):
        push(q, i, *arrivals(q)[i]).wait_recv()

    def own(q):
        for i in (0, 1, 2):
            start(q, i)

    def forward(q):
        for got, gives in ((0, (3, 4)), (1, (5, 10)), (2, (6, 9, 11)), (3, (7,)), (4, (8,)), (5, (12,)), (9, (13,))):
            take(q, got)
            for i in gives:
                start(q, i)

    def finish(q):
        for i in (6, 7, 8, 10, 11, 12, 13):
            take(q, i)

    mine = pltpu.make_async_copy(
        strip_ref, rows.at[pl.ds(pl.multiple_of(k * strip, PIECE), strip)], local_sem.at[0]
    )
    mine.start()

    def rhs_place(source):
        return resid.at[:, pl.ds(pl.multiple_of(source * cabs_local, PIECE), cabs_local)]

    keep = pltpu.make_async_copy(rhs_ref.at[k], rhs_place(k), local_sem.at[1])
    keep.start()

    barrier = pltpu.get_barrier_semaphore()
    for step in range(1, cols):
        pl.semaphore_signal(barrier, inc=1, device_id=(me, (k + step) % cols), device_id_type=MESH)
    for step in range(1, chains):
        pl.semaphore_signal(barrier, inc=1, device_id=((me + step) % chains, k), device_id_type=MESH)
    pl.semaphore_wait(barrier, cols + chains - 2)
    mine.wait()
    own(0)

    def rhs_copy(step, place):
        to = (k + step) % cols
        return pltpu.make_async_remote_copy(
            src_ref=rhs_ref.at[to], dst_ref=rhs_place(place),
            send_sem=rhs_send.at[step - 1], recv_sem=rhs_recv.at[step - 1],
            device_id=(me, to), device_id_type=MESH,
        )

    for step in range(1, cols):
        rhs_copy(step, k).start()

    pl.when(me >= 1)(lambda: own(1))
    forward(0)
    pl.when(me >= 2)(lambda: own(2))
    finish(0)

    diag_column = pl.multiple_of(me * aux, BLOCK)

    def diag(s, t, count=1):
        return rows[pl.ds(s * BLOCK, BLOCK), pl.ds(pl.multiple_of(diag_column + t * BLOCK, BLOCK), count * BLOCK)]

    row_id = lax.broadcasted_iota(jnp.int32, (BLOCK, BLOCK), 0)
    col_id = lax.broadcasted_iota(jnp.int32, (BLOCK, BLOCK), 1)
    for s in range(blocks):
        on = row_id == col_id
        inverse[s] = jnp.where(on, 1.0 / jnp.where(on, diag(s, s), 1.0), 0.0)

    def double(level, carry):
        low_row, low_col = row_id >> level, col_id >> level
        pick = ((low_row >> 1) == (low_col >> 1)) & (low_row > low_col)
        for s in range(blocks):
            off = jnp.where(pick, diag(s, s), 0.0)
            inverse[s] = inverse[s] - plain(inverse[s], plain(off, inverse[s]))
        return carry

    lax.fori_loop(0, BLOCK.bit_length() - 1, double, 0)

    keep.wait()
    for step in range(1, cols):
        rhs_copy(step, (k + cols - step) % cols).wait_recv()

    def chain_copy(section, step):
        to = (section + step) % chains
        return pltpu.make_async_remote_copy(
            src_ref=out_ref, dst_ref=solved.at[section],
            send_sem=chain_send.at[step - 1], recv_sem=chain_recv.at[section],
            device_id=(to, k), device_id_type=MESH,
        )

    tall = aux // 3 if aux % (3 * BLOCK) == 0 else BLOCK
    for q in range(1, chains):

        def section(q=q):
            forward(q)
            if q + 2 < chains + 0:
                pl.when(me >= q + 2)(lambda: own(q + 2))
            finish(q)
            chain_copy(q - 1, 1).wait_recv()
            arrived = solved[q - 1].reshape(width, aux)
            for m in range(aux // tall):
                part = pl.ds(m * tall, tall)
                change = times_t(arrived, rows[part, pl.ds((q - 1) * aux, aux)])
                resid[:, :, part] = resid[:, :, part] - change.reshape(resid.shape[0], resid.shape[1], tall)

        pl.when(me >= q)(section)

    shape = (out_ref.shape[0], out_ref.shape[1], BLOCK)
    for s in range(blocks):
        part = pl.ds(s * BLOCK, BLOCK)
        left = resid[:, :, part].reshape(width, BLOCK)
        if s:
            left = left - times_t(out_ref[:, :, : s * BLOCK].reshape(width, s * BLOCK), diag(s, 0, s))
        out_ref[:, :, part] = times_t(left, inverse[s]).reshape(shape)

    for section in range(chains - 1):

        def tell(section=section):
            for step in range(1, chains - section):
                chain_copy(section, step).start()
            for step in range(1, chains - section):
                chain_copy(section, step).wait_send()

        pl.when(me == section)(tell)

    for step in range(1, cols):
        rhs_copy(step, k).wait_send()
    for q in range(chains):

        def settle(q=q):
            for i, what in sends(q).items():
                push(q, i, *what).wait_send()

        pl.when(me >= q)(settle)


def gathered(chains, ring, factor, right_side, occ_order, cabs_order):
    cols = 2 * ring
    strip = factor.shape[0]
    aux = right_side.shape[0]
    occ_total, cabs_total = occ_order.shape[0], cabs_order.shape[0]
    cabs_local, occ_local = cabs_total // cols, occ_total // cols
    rhs = right_side.reshape(aux, cabs_local, occ_total).transpose(2, 1, 0)
    rhs = jnp.take(rhs, occ_order, axis=0).reshape(cols, occ_local, cabs_local, aux)
    dma = pltpu.SemaphoreType.DMA
    found = pl.pallas_call(
        functools.partial(kernel, chains, ring),
        out_shape=jax.ShapeDtypeStruct((occ_local, cabs_total, aux), jnp.float32),
        in_specs=[pl.BlockSpec(memory_space=pl.ANY)] * 2,
        out_specs=pl.BlockSpec(memory_space=pltpu.VMEM),
        scratch_shapes=[
            pltpu.VMEM((aux, factor.shape[1]), jnp.float32),
            pltpu.VMEM((occ_local, cabs_total, aux), jnp.float32),
            pltpu.VMEM((chains - 1, occ_local, cabs_total, aux), jnp.float32),
            pltpu.VMEM((aux // BLOCK, BLOCK, BLOCK), jnp.float32),
            dma((chains, 14)),
            dma((chains, 14)),
            dma((chains - 1,)),
            dma((chains - 1,)),
            dma((cols - 1,)),
            dma((cols - 1,)),
            dma((2,)),
        ],
        compiler_params=pltpu.CompilerParams(
            collective_id=0, has_side_effects=True, vmem_limit_bytes=56 * 1024 * 1024
        ),
    )(factor, rhs)
    return jnp.take(found, cabs_order, axis=1)


def solution(mesh):
    chains, cols = mesh.shape["chain"], mesh.shape["cols"]

    def per_device(factor, right_side, occ_order, cabs_order):
        tiled = factor.shape[0] % PIECE == 0 and right_side.shape[0] % BLOCK == 0
        if tiled and cols // 2 == 4 and (cabs_order.shape[0] // cols) % PIECE == 0:
            return gathered(chains, cols // 2, factor, right_side, occ_order, cabs_order)
        return general(factor, right_side, occ_order, cabs_order)

    in_specs = (P(("chain", "cols"), None), P("chain", "cols"), P(), P())
    out_specs = P("cols", None, "chain")
    return jax.shard_map(
        per_device, mesh=mesh, in_specs=in_specs, out_specs=out_specs, check_vma=False
    )
```

```python
import functools

import jax
import jax.numpy as jnp
from jax import lax
from jax.experimental import pallas as pl
from jax.experimental.pallas import tpu as pltpu
from jax.sharding import PartitionSpec as P

BLOCK = 128
PIECE = 8
MESH = pl.DeviceIdType.MESH


def from_root(value, axis, source):
    kept = jnp.where(lax.axis_index(axis) == source, value, 0).astype(value.dtype)
    return lax.psum(kept, axis)


def product(left, right):
    return jnp.dot(left, right, precision=lax.Precision.HIGHEST, preferred_element_type=jnp.float32)


def general(factor, right_side, occ_order, cabs_order):
    chain_size = lax.axis_size("chain")
    position = lax.axis_index("chain")
    factor_row = lax.all_gather(factor, "cols", axis=0, tiled=True)
    aux_rows = factor_row.shape[0]
    diag_block = lax.dynamic_slice_in_dim(factor_row, position * aux_rows, aux_rows, 1)
    identity = jnp.eye(aux_rows, dtype=jnp.float32)
    inverse = jax.scipy.linalg.solve_triangular(diag_block, identity, lower=True)

    def settle(residual):
        return product(inverse, residual)

    def blank(residual):
        return jnp.zeros_like(residual)

    residual = right_side
    solution = jnp.zeros_like(right_side)
    for section in range(chain_size):
        solved = lax.cond(position == section, settle, blank, residual)
        solution = solution + solved
        if section + 1 < chain_size:
            arrived = from_root(solved, "chain", section)
            coupling = factor_row[:, section * aux_rows : (section + 1) * aux_rows]

            def lower_block(current, arrived=arrived, coupling=coupling):
                return current - product(coupling, arrived)

            def keep_block(current):
                return current

            residual = lax.cond(position > section, lower_block, keep_block, residual)
    occ_total = occ_order.shape[0]
    cabs_local = right_side.shape[1] // occ_total
    cols_size = lax.axis_size("cols")
    occ_local = occ_total // cols_size
    grid = solution.reshape(aux_rows, cabs_local, occ_total)
    grid = jnp.take(grid, occ_order, axis=2)
    grid = grid.reshape(aux_rows, cabs_local, cols_size, occ_local)
    grid = jnp.transpose(grid, (2, 3, 1, 0))
    moved = jnp.take(
        lax.all_to_all(grid, "cols", split_axis=0, concat_axis=2, tiled=True), cabs_order, axis=2
    )
    return moved.reshape(occ_local, moved.shape[2], aux_rows)


def times_t(left, right, exact=False):
    precision = lax.Precision.HIGHEST
    dims = (((1,), (1,)), ((), ()))
    if exact:
        return lax.dot_general(left, right, dims, precision=precision, preferred_element_type=jnp.float32)
    left_hi = left.astype(jnp.bfloat16)
    left_lo = (left - left_hi.astype(jnp.float32)).astype(jnp.bfloat16)
    right_hi = right.astype(jnp.bfloat16)
    right_lo = (right - right_hi.astype(jnp.float32)).astype(jnp.bfloat16)
    dot = functools.partial(lax.dot_general, dimension_numbers=dims, preferred_element_type=jnp.float32)
    return dot(left_hi, right_hi) + (dot(left_hi, right_lo) + dot(left_lo, right_hi))


def plain(left, right):
    return jnp.dot(left, right, precision=lax.Precision.HIGHEST, preferred_element_type=jnp.float32)


def kernel(
    chains, ring, strip_ref, rhs_ref, out_ref, rows, resid, solved, found, inverse,
    up_send, down_send, line_recv, side_up_send, side_down_send, side_recv, cross_send, cross_recv,
    swap_send, swap_recv, chain_send, chain_recv, rhs_send, rhs_recv, out_sem, local_sem,
):
    cols = 2 * ring
    strip = strip_ref.shape[0]
    aux = strip * cols
    blocks = aux // BLOCK
    cabs_local = rhs_ref.shape[2]
    width = found.shape[0] * found.shape[1]
    me = lax.axis_index("chain")
    k = lax.axis_index("cols")
    z = k // 2
    x = k % 2
    partner = 2 * z + (1 - x)
    odd = me % 2
    even = me % 2 == 0
    peer = me + odd * (chains - 2 * me)
    role = peer

    def place_of(job):
        return job + (job % 2) * (chains - 2 * job)

    units = strip // PIECE
    side = (units + 3) // 6 * PIECE
    early = ((ring // 2 * 2 * strip + BLOCK - 1) // BLOCK) * BLOCK
    pieces = [(0, 0, early, 0), (0, early, aux - early, ring // 2)]
    pieces += [(q, 0, aux, 0) for q in range(1, chains)]

    def columns(p, job):
        q, begin, count, _ = pieces[p]
        start = job * aux if q == 0 else (q - 1) * aux
        return pl.ds(pl.multiple_of(start + begin, BLOCK), count)

    def slot(p, zz, xx, begin, size):
        start = pl.multiple_of((2 * zz + xx) * strip + begin, PIECE)
        return rows.at[pl.ds(start, size), columns(p, role)]

    def push(p, zz, xx, begin, size, send, recv, to):
        ref = slot(p, zz, xx, begin, size)
        return pltpu.make_async_remote_copy(
            src_ref=ref, dst_ref=ref, send_sem=send.at[p, zz], recv_sem=recv.at[p, zz],
            device_id=(me, to), device_id_type=MESH,
        )

    def line(p, zz, upward):
        send = up_send if upward else down_send
        return push(p, zz, x, 0, strip, send, line_recv, 2 * (z + 1 if upward else z - 1) + x)

    def aside(p, zz, upward):
        send = side_up_send if upward else side_down_send
        return push(p, zz, 1 - x, 0, side, send, side_recv, 2 * (z + 1 if upward else z - 1) + x)

    def cross(p, zz, xx, whole):
        begin = 0 if whole else side
        return push(p, zz, xx, begin, strip - begin, cross_send, cross_recv, partner)

    top = ring - 1

    def has(p, zz):
        return zz >= pieces[p][3]

    def own(p):
        @pl.when(has(p, z))
        def _():
            cross(p, z, x, True).start()
            pl.when(z < top)(lambda: line(p, z, True).start())
            pl.when(z > 0)(lambda: line(p, z, False).start())

    def from_below(p, d):
        return (z >= d) & has(p, z - d)

    def from_above(p, d):
        return (z + d <= top) & has(p, z + d)

    def forward(p, following):
        for d in range(1, ring):

            @pl.when(from_below(p, d))
            def _():
                line(p, z - d, True).wait_recv()
                pl.when(z < top)(lambda: line(p, z - d, True).start())
                cross(p, z - d, x, False).start()

            @pl.when(from_above(p, d))
            def _():
                line(p, z + d, False).wait_recv()
                pl.when(z > 0)(lambda: line(p, z + d, False).start())
                cross(p, z + d, x, False).start()

            if d == 1:

                @pl.when(has(p, z))
                def _():
                    cross(p, z, 1 - x, True).wait_recv()
                    pl.when(z < top)(lambda: aside(p, z, True).start())
                    pl.when(z > 0)(lambda: aside(p, z, False).start())

                following()

            @pl.when(from_below(p, d))
            def _():
                aside(p, z - d, True).wait_recv()
                pl.when(z < top)(lambda: aside(p, z - d, True).start())

            @pl.when(from_above(p, d))
            def _():
                aside(p, z + d, False).wait_recv()
                pl.when(z > 0)(lambda: aside(p, z + d, False).start())

    def finish(p):
        for d in range(1, ring):
            pl.when(from_below(p, d))(lambda: cross(p, z - d, 1 - x, False).wait_recv())
            pl.when(from_above(p, d))(lambda: cross(p, z + d, 1 - x, False).wait_recv())

    def settle(p):
        pl.when(has(p, z))(lambda: cross(p, z, x, True).wait_send())
        pl.when(has(p, z) & (z < top))(lambda: line(p, z, True).wait_send())
        pl.when(has(p, z) & (z > 0))(lambda: line(p, z, False).wait_send())
        pl.when(has(p, z) & (z < top))(lambda: aside(p, z, True).wait_send())
        pl.when(has(p, z) & (z > 0))(lambda: aside(p, z, False).wait_send())
        for d in range(1, ring):

            @pl.when(from_below(p, d))
            def _():
                cross(p, z - d, x, False).wait_send()

                @pl.when(z < top)
                def _():
                    line(p, z - d, True).wait_send()
                    aside(p, z - d, True).wait_send()

            @pl.when(from_above(p, d))
            def _():
                cross(p, z + d, x, False).wait_send()

                @pl.when(z > 0)
                def _():
                    line(p, z + d, False).wait_send()
                    aside(p, z + d, False).wait_send()

    mine = pl.ds(pl.multiple_of(k * strip, PIECE), strip)

    def load():
        return pltpu.make_async_copy(strip_ref, rows.at[mine], local_sem.at[0])

    def swap(p, job):
        return pltpu.make_async_remote_copy(
            src_ref=strip_ref.at[:, columns(p, job)], dst_ref=rows.at[mine, columns(p, job)],
            send_sem=swap_send.at[p], recv_sem=swap_recv.at[p],
            device_id=(peer, k), device_id_type=MESH,
        )

    def rhs_place(source):
        return resid.at[:, pl.ds(pl.multiple_of(source * cabs_local, PIECE), cabs_local)]

    def keep():
        return pltpu.make_async_copy(rhs_ref.at[k], rhs_place(k), local_sem.at[1])

    def rhs_copy(step, source):
        to = (k + step) % cols
        return pltpu.make_async_remote_copy(
            src_ref=rhs_ref.at[to], dst_ref=rhs_place(source),
            send_sem=rhs_send.at[step], recv_sem=rhs_recv.at[step],
            device_id=(peer, to), device_id_type=MESH,
        )

    @pl.when(even)
    def _():
        load().start()
        keep().start()

    barrier = pltpu.get_barrier_semaphore()
    for step in range(1, cols):
        pl.semaphore_signal(barrier, inc=1, device_id=(me, (k + step) % cols), device_id_type=MESH)
    for step in range(1, chains):
        pl.semaphore_signal(barrier, inc=1, device_id=((me + step) % chains, k), device_id_type=MESH)

    @pl.when(odd == 1)
    def _():
        for step in range(1, cols):
            pl.semaphore_signal(barrier, inc=1, device_id=(peer, (k + step) % cols), device_id_type=MESH)

    pl.semaphore_wait(barrier, cols + chains - 2 + odd * (cols - 1))

    @pl.when(odd == 1)
    def _():
        for p in range(len(pieces)):
            pl.when((me >= pieces[p][0]) & has(p, z))(lambda: swap(p, me).start())
        rhs_copy(0, k).start()

    def ready(p):
        pl.when((odd == 1) & has(p, z))(lambda: swap(p, role).wait_recv())
        own(p)

    pl.when(even)(lambda: load().wait())
    ready(0)
    for step in range(1, cols):
        rhs_copy(step, k).start()

    forward(0, lambda: ready(1))
    forward(1, lambda: pl.when(role >= 1)(lambda: ready(2)))
    finish(0)
    finish(1)

    diag_column = pl.multiple_of(role * aux, BLOCK)

    def diag(s, t, count=1):
        return rows[pl.ds(s * BLOCK, BLOCK), pl.ds(pl.multiple_of(diag_column + t * BLOCK, BLOCK), count * BLOCK)]

    row_id = lax.broadcasted_iota(jnp.int32, (BLOCK, BLOCK), 0)
    col_id = lax.broadcasted_iota(jnp.int32, (BLOCK, BLOCK), 1)
    for s in range(blocks):
        on = row_id == col_id
        inverse[s] = jnp.where(on, 1.0 / jnp.where(on, diag(s, s), 1.0), 0.0)

    def double(level, carry):
        low_row, low_col = row_id >> level, col_id >> level
        pick = ((low_row >> 1) == (low_col >> 1)) & (low_row > low_col)
        for s in range(blocks):
            off = jnp.where(pick, diag(s, s), 0.0)
            inverse[s] = inverse[s] - plain(inverse[s], plain(off, inverse[s]))
        return carry

    lax.fori_loop(0, BLOCK.bit_length() - 1, double, 0)

    pl.when(even)(lambda: keep().wait())
    pl.when(odd == 1)(lambda: rhs_copy(0, k).wait_recv())
    for step in range(1, cols):
        rhs_copy(step, (k + cols - step) % cols).wait_recv()

    def chain_copy(section, step):
        return pltpu.make_async_remote_copy(
            src_ref=found, dst_ref=solved.at[section],
            send_sem=chain_send.at[step - 1], recv_sem=chain_recv.at[section],
            device_id=(place_of((section + step) % chains), k), device_id_type=MESH,
        )

    tall = aux // 3 if aux % (3 * BLOCK) == 0 else BLOCK
    for q in range(1, chains):

        def section(q=q):
            p = q + 1
            following = (lambda: pl.when(role >= q + 1)(lambda: ready(p + 1))) if q + 1 < chains else (lambda: None)
            forward(p, following)
            finish(p)
            chain_copy(q - 1, 1).wait_recv()
            arrived = solved[q - 1].reshape(width, aux)
            for m in range(aux // tall):
                part = pl.ds(m * tall, tall)
                change = times_t(arrived, rows[part, pl.ds((q - 1) * aux, aux)])
                resid[:, :, part] = resid[:, :, part] - change.reshape(resid.shape[0], resid.shape[1], tall)

        pl.when(role >= q)(section)

    shape = (found.shape[0], found.shape[1], BLOCK)
    for s in range(blocks):
        part = pl.ds(s * BLOCK, BLOCK)
        left = resid[:, :, part].reshape(width, BLOCK)
        if s:
            left = left - times_t(found[:, :, : s * BLOCK].reshape(width, s * BLOCK), diag(s, 0, s))
        found[:, :, part] = times_t(left, inverse[s]).reshape(shape)

    def give():
        return pltpu.make_async_remote_copy(
            src_ref=found, dst_ref=out_ref, send_sem=out_sem.at[0], recv_sem=out_sem.at[1],
            device_id=(peer, k), device_id_type=MESH,
        )

    def put():
        return pltpu.make_async_copy(found, out_ref, local_sem.at[0])

    for section in range(chains - 1):

        def tell(section=section):
            for step in range(1, chains - section):
                chain_copy(section, step).start()
            for step in range(1, chains - section):
                chain_copy(section, step).wait_send()

        pl.when(role == section)(tell)

    pl.when(odd == 1)(lambda: give().start())
    pl.when(even)(lambda: put().start())
    for step in range(1, cols):
        rhs_copy(step, k).wait_send()
    for p in range(len(pieces)):
        pl.when(role >= pieces[p][0])(lambda: settle(p))

    @pl.when(odd == 1)
    def _():
        rhs_copy(0, k).wait_send()
        for p in range(len(pieces)):
            pl.when((me >= pieces[p][0]) & has(p, z))(lambda: swap(p, me).wait_send())
        give().wait_send()
        give().wait_recv()

    pl.when(even)(lambda: put().wait())


def gathered(chains, ring, factor, right_side, occ_order, cabs_order):
    cols = 2 * ring
    strip = factor.shape[0]
    aux = right_side.shape[0]
    occ_total, cabs_total = occ_order.shape[0], cabs_order.shape[0]
    cabs_local, occ_local = cabs_total // cols, occ_total // cols
    rhs = right_side.reshape(aux, cabs_local, occ_total).transpose(2, 1, 0)
    rhs = jnp.take(rhs, occ_order, axis=0).reshape(cols, occ_local, cabs_local, aux)
    dma = pltpu.SemaphoreType.DMA
    found = pl.pallas_call(
        functools.partial(kernel, chains, ring),
        out_shape=jax.ShapeDtypeStruct((occ_local, cabs_total, aux), jnp.float32),
        in_specs=[pl.BlockSpec(memory_space=pl.ANY)] * 2,
        out_specs=pl.BlockSpec(memory_space=pl.ANY),
        scratch_shapes=[
            pltpu.VMEM((aux, factor.shape[1]), jnp.float32),
            pltpu.VMEM((occ_local, cabs_total, aux), jnp.float32),
            pltpu.VMEM((chains - 1, occ_local, cabs_total, aux), jnp.float32),
            pltpu.VMEM((occ_local, cabs_total, aux), jnp.float32),
            pltpu.VMEM((aux // BLOCK, BLOCK, BLOCK), jnp.float32),
            *[dma((chains + 1, ring)) for _ in range(8)],
            dma((chains + 1,)),
            dma((chains + 1,)),
            dma((chains - 1,)),
            dma((chains - 1,)),
            dma((cols,)),
            dma((cols,)),
            dma((2,)),
            dma((2,)),
        ],
        compiler_params=pltpu.CompilerParams(
            collective_id=0, has_side_effects=True, vmem_limit_bytes=56 * 1024 * 1024
        ),
    )(factor, rhs)
    return jnp.take(found, cabs_order, axis=1)


def solution(mesh):
    chains, cols = mesh.shape["chain"], mesh.shape["cols"]

    def per_device(factor, right_side, occ_order, cabs_order):
        tiled = factor.shape[0] % PIECE == 0 and right_side.shape[0] % BLOCK == 0
        if tiled and cols // 2 == 4 and chains == 4 and (cabs_order.shape[0] // cols) % PIECE == 0:
            return gathered(chains, cols // 2, factor, right_side, occ_order, cabs_order)
        return general(factor, right_side, occ_order, cabs_order)

    in_specs = (P(("chain", "cols"), None), P("chain", "cols"), P(), P())
    out_specs = P("cols", None, "chain")
    return jax.shard_map(
        per_device, mesh=mesh, in_specs=in_specs, out_specs=out_specs, check_vma=False
    )
```

```python
import functools

import jax
import jax.numpy as jnp
from jax import lax
from jax.experimental import pallas as pl
from jax.experimental.pallas import tpu as pltpu
from jax.sharding import PartitionSpec as P

BLOCK = 128
PIECE = 8
AHEAD = 3
MESH = pl.DeviceIdType.MESH


def from_root(value, axis, source):
    kept = jnp.where(lax.axis_index(axis) == source, value, 0).astype(value.dtype)
    return lax.psum(kept, axis)


def product(left, right):
    return jnp.dot(left, right, precision=lax.Precision.HIGHEST, preferred_element_type=jnp.float32)


def general(factor, right_side, occ_order, cabs_order):
    chain_size = lax.axis_size("chain")
    position = lax.axis_index("chain")
    factor_row = lax.all_gather(factor, "cols", axis=0, tiled=True)
    aux_rows = factor_row.shape[0]
    diag_block = lax.dynamic_slice_in_dim(factor_row, position * aux_rows, aux_rows, 1)
    identity = jnp.eye(aux_rows, dtype=jnp.float32)
    inverse = jax.scipy.linalg.solve_triangular(diag_block, identity, lower=True)

    def settle(residual):
        return product(inverse, residual)

    def blank(residual):
        return jnp.zeros_like(residual)

    residual = right_side
    solution = jnp.zeros_like(right_side)
    for section in range(chain_size):
        solved = lax.cond(position == section, settle, blank, residual)
        solution = solution + solved
        if section + 1 < chain_size:
            arrived = from_root(solved, "chain", section)
            coupling = factor_row[:, section * aux_rows : (section + 1) * aux_rows]

            def lower_block(current, arrived=arrived, coupling=coupling):
                return current - product(coupling, arrived)

            def keep_block(current):
                return current

            residual = lax.cond(position > section, lower_block, keep_block, residual)
    occ_total = occ_order.shape[0]
    cabs_local = right_side.shape[1] // occ_total
    cols_size = lax.axis_size("cols")
    occ_local = occ_total // cols_size
    grid = solution.reshape(aux_rows, cabs_local, occ_total)
    grid = jnp.take(grid, occ_order, axis=2)
    grid = grid.reshape(aux_rows, cabs_local, cols_size, occ_local)
    grid = jnp.transpose(grid, (2, 3, 1, 0))
    moved = jnp.take(
        lax.all_to_all(grid, "cols", split_axis=0, concat_axis=2, tiled=True), cabs_order, axis=2
    )
    return moved.reshape(occ_local, moved.shape[2], aux_rows)


def times_t(left, right, exact=False):
    precision = lax.Precision.HIGHEST
    dims = (((1,), (1,)), ((), ()))
    if exact:
        return lax.dot_general(left, right, dims, precision=precision, preferred_element_type=jnp.float32)
    left_hi = left.astype(jnp.bfloat16)
    left_lo = (left - left_hi.astype(jnp.float32)).astype(jnp.bfloat16)
    right_hi = right.astype(jnp.bfloat16)
    right_lo = (right - right_hi.astype(jnp.float32)).astype(jnp.bfloat16)
    dot = functools.partial(lax.dot_general, dimension_numbers=dims, preferred_element_type=jnp.float32)
    return dot(left_hi, right_hi) + (dot(left_hi, right_lo) + dot(left_lo, right_hi))


def plain(left, right):
    return jnp.dot(left, right, precision=lax.Precision.HIGHEST, preferred_element_type=jnp.float32)


def kernel(
    chains, ring, strip_ref, rhs_ref, out_ref, rows, resid, solved, found, inverse,
    up_send, down_send, line_recv, side_up_send, side_down_send, side_recv, cross_send, cross_recv,
    swap_send, swap_recv, chain_send, chain_recv, rhs_send, rhs_recv, out_sem, local_sem,
):
    cols = 2 * ring
    strip = strip_ref.shape[0]
    aux = strip * cols
    blocks = aux // BLOCK
    cabs_local = rhs_ref.shape[2]
    width = found.shape[0] * found.shape[1]
    me = lax.axis_index("chain")
    k = lax.axis_index("cols")
    z = k // 2
    x = k % 2
    partner = 2 * z + (1 - x)
    odd = me % 2
    even = me % 2 == 0
    peer = me + odd * (chains - 2 * me)
    role = peer

    def place_of(job):
        return job + (job % 2) * (chains - 2 * job)

    units = strip // PIECE
    side = (units + 3) // 6 * PIECE
    early = ((ring // 2 * 2 * strip + BLOCK - 1) // BLOCK) * BLOCK
    pieces = [(0, 0, early, 0), (0, early, aux - early, ring // 2)]
    for q in range(1, chains):
        pieces += [(q, 0, early, 0), (q, early, aux - early, 0)]

    def columns(p, job):
        q, begin, count, _ = pieces[p]
        start = job * aux if q == 0 else (q - 1) * aux
        return pl.ds(pl.multiple_of(start + begin, BLOCK), count)

    def slot(p, zz, xx, begin, size):
        start = pl.multiple_of((2 * zz + xx) * strip + begin, PIECE)
        return rows.at[pl.ds(start, size), columns(p, role)]

    def push(p, zz, xx, begin, size, send, recv, to):
        ref = slot(p, zz, xx, begin, size)
        return pltpu.make_async_remote_copy(
            src_ref=ref, dst_ref=ref, send_sem=send.at[p, zz], recv_sem=recv.at[p, zz],
            device_id=(me, to), device_id_type=MESH,
        )

    def line(p, zz, upward):
        send = up_send if upward else down_send
        return push(p, zz, x, 0, strip, send, line_recv, 2 * (z + 1 if upward else z - 1) + x)

    def aside(p, zz, upward):
        send = side_up_send if upward else side_down_send
        return push(p, zz, 1 - x, 0, side, send, side_recv, 2 * (z + 1 if upward else z - 1) + x)

    def cross(p, zz, xx, whole):
        begin = 0 if whole else side
        return push(p, zz, xx, begin, strip - begin, cross_send, cross_recv, partner)

    top = ring - 1

    def has(p, zz):
        return zz >= pieces[p][3]

    def own(p):
        @pl.when(has(p, z))
        def _():
            cross(p, z, x, True).start()
            pl.when(z < top)(lambda: line(p, z, True).start())
            pl.when(z > 0)(lambda: line(p, z, False).start())

    def from_below(p, d):
        return (z >= d) & has(p, z - d)

    def from_above(p, d):
        return (z + d <= top) & has(p, z + d)

    def stage(p, d):

        @pl.when(from_below(p, d))
        def _():
            line(p, z - d, True).wait_recv()
            pl.when(z < top)(lambda: line(p, z - d, True).start())
            cross(p, z - d, x, False).start()

        @pl.when(from_above(p, d))
        def _():
            line(p, z + d, False).wait_recv()
            pl.when(z > 0)(lambda: line(p, z + d, False).start())
            cross(p, z + d, x, False).start()

        if d == 1:

            @pl.when(has(p, z))
            def _():
                cross(p, z, 1 - x, True).wait_recv()
                pl.when(z < top)(lambda: aside(p, z, True).start())
                pl.when(z > 0)(lambda: aside(p, z, False).start())

        @pl.when(from_below(p, d))
        def _():
            aside(p, z - d, True).wait_recv()
            pl.when(z < top)(lambda: aside(p, z - d, True).start())

        @pl.when(from_above(p, d))
        def _():
            aside(p, z + d, False).wait_recv()
            pl.when(z > 0)(lambda: aside(p, z + d, False).start())

    def finish(p):
        for d in range(1, ring):
            pl.when(from_below(p, d))(lambda: cross(p, z - d, 1 - x, False).wait_recv())
            pl.when(from_above(p, d))(lambda: cross(p, z + d, 1 - x, False).wait_recv())

    def settle(p):
        pl.when(has(p, z))(lambda: cross(p, z, x, True).wait_send())
        pl.when(has(p, z) & (z < top))(lambda: line(p, z, True).wait_send())
        pl.when(has(p, z) & (z > 0))(lambda: line(p, z, False).wait_send())
        pl.when(has(p, z) & (z < top))(lambda: aside(p, z, True).wait_send())
        pl.when(has(p, z) & (z > 0))(lambda: aside(p, z, False).wait_send())
        for d in range(1, ring):

            @pl.when(from_below(p, d))
            def _():
                cross(p, z - d, x, False).wait_send()

                @pl.when(z < top)
                def _():
                    line(p, z - d, True).wait_send()
                    aside(p, z - d, True).wait_send()

            @pl.when(from_above(p, d))
            def _():
                cross(p, z + d, x, False).wait_send()

                @pl.when(z > 0)
                def _():
                    line(p, z + d, False).wait_send()
                    aside(p, z + d, False).wait_send()

    mine = pl.ds(pl.multiple_of(k * strip, PIECE), strip)

    def load():
        return pltpu.make_async_copy(strip_ref, rows.at[mine], local_sem.at[0])

    def swap(p, job):
        return pltpu.make_async_remote_copy(
            src_ref=strip_ref.at[:, columns(p, job)], dst_ref=rows.at[mine, columns(p, job)],
            send_sem=swap_send.at[p], recv_sem=swap_recv.at[p],
            device_id=(peer, k), device_id_type=MESH,
        )

    def rhs_place(source):
        return resid.at[:, pl.ds(pl.multiple_of(source * cabs_local, PIECE), cabs_local)]

    def keep():
        return pltpu.make_async_copy(rhs_ref.at[k], rhs_place(k), local_sem.at[1])

    def rhs_copy(step, source):
        to = (k + step) % cols
        return pltpu.make_async_remote_copy(
            src_ref=rhs_ref.at[to], dst_ref=rhs_place(source),
            send_sem=rhs_send.at[step], recv_sem=rhs_recv.at[step],
            device_id=(peer, to), device_id_type=MESH,
        )

    @pl.when(even)
    def _():
        load().start()
        keep().start()

    barrier = pltpu.get_barrier_semaphore()
    for step in range(1, cols):
        pl.semaphore_signal(barrier, inc=1, device_id=(me, (k + step) % cols), device_id_type=MESH)
    for step in range(1, chains):
        pl.semaphore_signal(barrier, inc=1, device_id=((me + step) % chains, k), device_id_type=MESH)

    @pl.when(odd == 1)
    def _():
        for step in range(1, cols):
            pl.semaphore_signal(barrier, inc=1, device_id=(peer, (k + step) % cols), device_id_type=MESH)

    pl.semaphore_wait(barrier, cols + chains - 2 + odd * (cols - 1))

    @pl.when(odd == 1)
    def _():
        for p in range(len(pieces)):
            pl.when((me >= pieces[p][0]) & has(p, z))(lambda: swap(p, me).start())
        rhs_copy(0, k).start()

    def ready(p):
        pl.when((odd == 1) & has(p, z))(lambda: swap(p, role).wait_recv())
        own(p)

    pl.when(even)(lambda: load().wait())
    ready(0)
    for step in range(1, cols):
        rhs_copy(step, k).start()
    for p in range(1, AHEAD):
        pl.when(role >= pieces[p][0])(lambda: ready(p))

    diag_column = pl.multiple_of(role * aux, BLOCK)

    def diag(s, t, count=1):
        return rows[pl.ds(s * BLOCK, BLOCK), pl.ds(pl.multiple_of(diag_column + t * BLOCK, BLOCK), count * BLOCK)]

    row_id = lax.broadcasted_iota(jnp.int32, (BLOCK, BLOCK), 0)
    col_id = lax.broadcasted_iota(jnp.int32, (BLOCK, BLOCK), 1)
    def double(level, carry):
        low_row, low_col = row_id >> level, col_id >> level
        pick = ((low_row >> 1) == (low_col >> 1)) & (low_row > low_col)
        for s in range(blocks):
            off = jnp.where(pick, diag(s, s), 0.0)
            inverse[s] = inverse[s] - plain(inverse[s], plain(off, inverse[s]))
        return carry

    def chain_copy(section, step):
        return pltpu.make_async_remote_copy(
            src_ref=found, dst_ref=solved.at[section],
            send_sem=chain_send.at[step - 1], recv_sem=chain_recv.at[section],
            device_id=(place_of((section + step) % chains), k), device_id_type=MESH,
        )

    tall = aux // 3 if aux % (3 * BLOCK) == 0 else BLOCK

    def invert():
        for s in range(blocks):
            on = row_id == col_id
            inverse[s] = jnp.where(on, 1.0 / jnp.where(on, diag(s, s), 1.0), 0.0)
        lax.fori_loop(0, BLOCK.bit_length() - 1, double, 0)
        pl.when(even)(lambda: keep().wait())
        pl.when(odd == 1)(lambda: rhs_copy(0, k).wait_recv())
        for step in range(1, cols):
            rhs_copy(step, (k + cols - step) % cols).wait_recv()

    def update(q):
        chain_copy(q - 1, 1).wait_recv()
        arrived = solved[q - 1].reshape(width, aux)
        for m in range(aux // tall):
            part = pl.ds(m * tall, tall)
            change = times_t(arrived, rows[part, pl.ds((q - 1) * aux, aux)])
            resid[:, :, part] = resid[:, :, part] - change.reshape(resid.shape[0], resid.shape[1], tall)

    def consume(p):
        finish(p)
        if p == 1:
            invert()
        if p > 1 and pieces[p][1]:
            update(pieces[p][0])

    def present(p):
        return role >= pieces[p][0]

    for t in range(len(pieces) + ring - 1):
        for d in range(1, ring):
            p = t - d + 1
            if 0 <= p < len(pieces):
                pl.when(present(p))(lambda: stage(p, d))
            if d == 1 and t + AHEAD < len(pieces):
                pl.when(present(t + AHEAD))(lambda: ready(t + AHEAD))
        if t >= ring - 1:
            p = t - ring + 1
            pl.when(present(p))(lambda: consume(p))

    shape = (found.shape[0], found.shape[1], BLOCK)
    for s in range(blocks):
        part = pl.ds(s * BLOCK, BLOCK)
        left = resid[:, :, part].reshape(width, BLOCK)
        if s:
            left = left - times_t(found[:, :, : s * BLOCK].reshape(width, s * BLOCK), diag(s, 0, s))
        found[:, :, part] = times_t(left, inverse[s]).reshape(shape)

    def give():
        return pltpu.make_async_remote_copy(
            src_ref=found, dst_ref=out_ref, send_sem=out_sem.at[0], recv_sem=out_sem.at[1],
            device_id=(peer, k), device_id_type=MESH,
        )

    def put():
        return pltpu.make_async_copy(found, out_ref, local_sem.at[0])

    for section in range(chains - 1):

        def tell(section=section):
            for step in range(1, chains - section):
                chain_copy(section, step).start()
            for step in range(1, chains - section):
                chain_copy(section, step).wait_send()

        pl.when(role == section)(tell)

    pl.when(odd == 1)(lambda: give().start())
    pl.when(even)(lambda: put().start())
    for step in range(1, cols):
        rhs_copy(step, k).wait_send()
    for p in range(len(pieces)):
        pl.when(role >= pieces[p][0])(lambda: settle(p))

    @pl.when(odd == 1)
    def _():
        rhs_copy(0, k).wait_send()
        for p in range(len(pieces)):
            pl.when((me >= pieces[p][0]) & has(p, z))(lambda: swap(p, me).wait_send())
        give().wait_send()
        give().wait_recv()

    pl.when(even)(lambda: put().wait())


def gathered(chains, ring, factor, right_side, occ_order, cabs_order):
    cols = 2 * ring
    strip = factor.shape[0]
    aux = right_side.shape[0]
    occ_total, cabs_total = occ_order.shape[0], cabs_order.shape[0]
    cabs_local, occ_local = cabs_total // cols, occ_total // cols
    rhs = right_side.reshape(aux, cabs_local, occ_total).transpose(2, 1, 0)
    rhs = jnp.take(rhs, occ_order, axis=0).reshape(cols, occ_local, cabs_local, aux)
    dma = pltpu.SemaphoreType.DMA
    found = pl.pallas_call(
        functools.partial(kernel, chains, ring),
        out_shape=jax.ShapeDtypeStruct((occ_local, cabs_total, aux), jnp.float32),
        in_specs=[pl.BlockSpec(memory_space=pl.ANY)] * 2,
        out_specs=pl.BlockSpec(memory_space=pl.ANY),
        scratch_shapes=[
            pltpu.VMEM((aux, factor.shape[1]), jnp.float32),
            pltpu.VMEM((occ_local, cabs_total, aux), jnp.float32),
            pltpu.VMEM((chains - 1, occ_local, cabs_total, aux), jnp.float32),
            pltpu.VMEM((occ_local, cabs_total, aux), jnp.float32),
            pltpu.VMEM((aux // BLOCK, BLOCK, BLOCK), jnp.float32),
            *[dma((2 * chains, ring)) for _ in range(8)],
            dma((2 * chains,)),
            dma((2 * chains,)),
            dma((chains - 1,)),
            dma((chains - 1,)),
            dma((cols,)),
            dma((cols,)),
            dma((2,)),
            dma((2,)),
        ],
        compiler_params=pltpu.CompilerParams(
            collective_id=0, has_side_effects=True, vmem_limit_bytes=56 * 1024 * 1024
        ),
    )(factor, rhs)
    return jnp.take(found, cabs_order, axis=1)


def solution(mesh):
    chains, cols = mesh.shape["chain"], mesh.shape["cols"]

    def per_device(factor, right_side, occ_order, cabs_order):
        tiled = factor.shape[0] % PIECE == 0 and right_side.shape[0] % BLOCK == 0
        if tiled and cols // 2 == 4 and chains == 4 and (cabs_order.shape[0] // cols) % PIECE == 0:
            return gathered(chains, cols // 2, factor, right_side, occ_order, cabs_order)
        return general(factor, right_side, occ_order, cabs_order)

    in_specs = (P(("chain", "cols"), None), P("chain", "cols"), P(), P())
    out_specs = P("cols", None, "chain")
    return jax.shard_map(
        per_device, mesh=mesh, in_specs=in_specs, out_specs=out_specs, check_vma=False
    )
```
